32 devices in a mesh: dp: 4 (over x, core), vocab: 8 (over z, y).
Axes of the slice: x: 2, y: 2, z: 4, core: 2. Of those that a mesh axis runs over, the one named last changes fastest.
Arguments:
- hidden: bfloat16 [128, 8192], P(('dp', 'vocab')), may hold values from -350 to 350
- lm_head: bfloat16 [8192, 128256], P(None, ('dp', 'vocab')), may hold values from -0.0625 to 0.0625
- targets: int32 [128], P(('dp', 'vocab')), may hold values from 0 to 128255
- segment: int32 [128], P(('dp', 'vocab')), may hold values from 0 to 32, as said below
- pad_mask: int32 [128], P(('dp', 'vocab')), may hold values from 0 to 1, as said below
- seq_bench: int32 [33], replicated, may hold values from 0 to 7
Outputs:
- token_nll: float32 [128], P(('dp', 'vocab'))
- bench_total: float32 [8], replicated
- bench_count: float32 [8], replicated
The draws below stay inside these ranges and needn't reach their ends.
Inputs may be any that keep to these rules, and one draw needn't show every extreme that they name: `segment`: sequence numbers never fall along the pack; each aligned block of 4 tokens holds exactly one place inside it where the number rises by one, and the number does not change between one block's last token and the next block's first. `pad_mask`: the last token of each aligned block of 4 tokens is real.
All inputs are finite; a program needn't handle non-finite values.
Results may differ from the reference program's by a relative error of at most 0.0003.
Values may be sent and summed in bfloat16 or wider, within the bound.
No kernel may reach another device: no remote copies, remote signals or barrier semaphores. Data moves between devices by JAX's collectives and lax.ppermute only.
A program may use at most 128 MiB of HBM per device.

```python
import math
import jax
import jax.numpy as jnp
import numpy as np
from jax import lax

D = 8192
VOCAB = 128256
TOK_DEV = 4
NBENCH = 8
TOKENS = 128
NSEQ = 33


def draw_hidden(key, part):
    first, second = jax.random.split(key, 2)
    base = jnp.clip(jax.random.normal(first, (TOKENS, D), jnp.float32), -5.0, 5.0)
    scales = 3.0 * jnp.exp(jax.random.uniform(second, (TOKENS,), jnp.float32, -0.3, 0.3))
    return (base * scales[:, None]).astype(jnp.bfloat16)


def draw_segment(key, part):
    blocks = TOKENS // TOK_DEV
    places = jax.random.randint(jax.random.fold_in(key, 11), (blocks,), 1, TOK_DEV)
    local = jnp.arange(TOK_DEV, dtype=jnp.int32)
    rises = (local[None, :] >= places[:, None]).astype(jnp.int32)
    numbers = jnp.arange(blocks, dtype=jnp.int32)[:, None] + rises
    return numbers.reshape(TOKENS).astype(jnp.int32)


def draw_pad_mask(key, part):
    blocks = TOKENS // TOK_DEV
    values = jax.random.randint(jax.random.fold_in(key, 23), (blocks, TOK_DEV), 0, 4)
    real = (values != 0).astype(jnp.int32)
    last = (jnp.arange(TOK_DEV, dtype=jnp.int32) == TOK_DEV - 1).astype(jnp.int32)
    return jnp.maximum(real, last[None, :]).reshape(TOKENS).astype(jnp.int32)


def place_ends(values, rng, smallest, top_value):
    dims = values.shape
    place = [jax.random.randint(jax.random.fold_in(rng, axis), (), 0, dims[axis]) for axis in range(len(dims))]
    values = values.at[tuple(place)].set(smallest)
    longest = dims.index(max(dims))
    place[longest] = (place[longest] + 1) % dims[longest]
    return values.at[tuple(place)].set(top_value)


def block_scale(stream_key, dims, cuts, least, largest):
    def one(axis_at, parts):
        steps = jax.random.uniform(jax.random.fold_in(jax.random.fold_in(stream_key, 6), axis_at), (parts,), jnp.float32, least / len(cuts), largest / len(cuts))
        return jnp.repeat(jnp.exp(steps), dims[axis_at] // parts).reshape((-1,) + (1,) * (len(dims) - axis_at - 1))

    loudness = one(*cuts[0])
    for cut in cuts[1:]:
        loudness = loudness * one(*cut)
    return loudness


def wide_ids(rng, extent, amount, lean):
    loads = [min(1 << octave, amount + 1 - (1 << octave)) * (1 << 20) // math.isqrt((1 << octave) ** lean) + 1 for octave in range((amount + 1).bit_length()) if 1 << octave <= amount]
    width = 1 + sum(loads) // (1 << 30)
    listing = np.cumsum(np.array([max(1, weight // width) for weight in loads]))
    ticket = jax.random.randint(jax.random.fold_in(rng, 1), extent, 0, int(listing[len(loads) - 1]))
    start = jnp.left_shift(1, jnp.searchsorted(jnp.asarray(listing, jnp.int32), ticket, side="right").astype(jnp.int32))
    rank = start - 1 + jax.random.randint(jax.random.fold_in(rng, 4), extent, 0, 1 << 30) % jnp.minimum(start, amount + 1 - start)
    return jax.random.permutation(jax.random.fold_in(rng, 2), amount)[rank].astype(jnp.int32)


def scatter_about(stream_key, dims, scale, most, pieces=(), held_as=jnp.bfloat16):
    drawn = scale * jax.random.normal(stream_key, dims, jnp.float32)
    if pieces:
        drawn = drawn * block_scale(stream_key, dims, pieces, -0.22, 0.18)
    return jnp.clip(drawn, -most, most).astype(held_as)


def setup_inputs(seed: int = 0) -> dict:
    seeds = jax.random.split(jax.random.key(seed), 7)
    return {
        "hidden": draw_hidden(jax.random.fold_in(seeds[6], 71), 0),
        "lm_head": scatter_about(seeds[1], (D, VOCAB), D ** -0.5, 0.0625, ((1, 32),)),
        "targets": place_ends(wide_ids(seeds[2], (TOKENS,), VOCAB, 2), jax.random.fold_in(seeds[2], 3), 0, VOCAB - 1).astype(jnp.int32),
        "segment": draw_segment(jax.random.fold_in(seeds[6], 71), 0),
        "pad_mask": draw_pad_mask(jax.random.fold_in(seeds[6], 71), 0),
        "seq_bench": place_ends(jax.random.randint(seeds[5], (NSEQ,), 0, NBENCH), jax.random.fold_in(seeds[5], 1), 0, NBENCH - 1).astype(jnp.int32),
    }


def reference(hidden, lm_head, targets, segment, pad_mask, seq_bench):
    block = math.gcd(TOKENS, 128)

    def one_block(pair):
        rows, wanted = pair
        logits = jnp.dot(rows, lm_head, preferred_element_type=jnp.float32)
        top = jnp.max(logits, axis=1)
        total = jnp.sum(jnp.exp(logits - top[:, None]), axis=1)
        picked = jnp.take_along_axis(logits, wanted[:, None], axis=1)[:, 0]
        return top + jnp.log(total) - picked

    token_nll = lax.map(one_block, (hidden.reshape(TOKENS // block, block, D), targets.reshape(TOKENS // block, block))).reshape(TOKENS)
    following = jnp.concatenate([segment[1:], jnp.full((1,), -1, jnp.int32)])
    keep = (pad_mask * (segment == following).astype(jnp.int32)).astype(jnp.float32)
    bench = seq_bench[segment]
    bench_hot = (bench[:, None] == jnp.arange(NBENCH, dtype=jnp.int32)[None, :]).astype(jnp.float32)
    bench_total = jnp.sum(bench_hot * (keep * token_nll)[:, None], axis=0)
    bench_count = jnp.sum(bench_hot * keep[:, None], axis=0)
    return token_nll, bench_total, bench_count
```

```python
from functools import partial

import jax
import jax.numpy as jnp
from jax import lax
from jax.experimental import pallas as pl
from jax.experimental.pallas import tpu as pltpu
from jax.sharding import PartitionSpec as P

NBENCH = 8
AXES = ("dp", "vocab")
LANES = 128
ROWS = 16
KTILE = 512


def swap(value, axis, bit):
    count = lax.axis_size(axis)
    return lax.ppermute(value, axis, [(i, i ^ bit) for i in range(count)])


def bits_from(low, count):
    out = []
    while low < count:
        out.append(low)
        low *= 2
    return out


def doubling(value, rounds):
    for axis, bit in rounds:
        value = jnp.concatenate([value, swap(value, axis, bit)], axis=0)
    return value


def gather_orders(n_dp, n_voc):
    far = [("vocab", b) for b in bits_from(2, n_voc)]
    side = [("dp", b) for b in bits_from(2, n_dp)]
    near = [("vocab", 1)]
    core = [("dp", 1)]
    return far + side + near + core, far + near + side + core


def gather_half(part, rounds, packed):
    rows, width = part.shape
    value = doubling(part.reshape(1, rows * width // LANES, LANES), rounds[:packed])
    value = value.reshape(1, rows * value.shape[0], width)
    return doubling(value, rounds[packed:])


def digit(value, place):
    return (lax.shift_right_logical(value, 8 * place) & 255).astype(jnp.bfloat16)


def logits_kernel(perm, positions, tok_dev, steps_a, me_ref, xa_ref, xb_ref, meta_ref, w_ref, out_ref, x_ref, acc_ref):
    step = pl.program_id(0)
    blocks = xa_ref.shape[0]
    tokens = x_ref.shape[0]

    @pl.when(step < steps_a)
    def _():
        for i in range(blocks):
            x_ref[i * ROWS : (i + 1) * ROWS, :] = xa_ref[i]

    @pl.when(step >= steps_a)
    def _():
        for i in range(blocks):
            x_ref[i * ROWS : (i + 1) * ROWS, :] = xb_ref[perm[i]]

    product = lax.dot_general(
        x_ref[...], w_ref[...], (((1,), (1,)), ((), ())), preferred_element_type=jnp.float32
    )

    @pl.when(step == 0)
    def _():
        acc_ref[...] = product

    @pl.when(step > 0)
    def _():
        acc_ref[...] += product

    @pl.when(step == pl.num_programs(0) - 1)
    def _():
        me = me_ref[0]
        logits = acc_ref[...]
        top = jnp.max(logits, axis=1, keepdims=True)
        total = jnp.sum(jnp.exp(logits - top), axis=1, keepdims=True)
        meta = meta_ref[...].reshape(tokens, LANES).astype(jnp.float32)
        target = meta[:, 0:1] + 256.0 * meta[:, 1:2] + 65536.0 * meta[:, 2:3]
        wanted = target.astype(jnp.int32) - me * logits.shape[1]
        columns = lax.broadcasted_iota(jnp.int32, logits.shape, 1)
        picked = jnp.sum(jnp.where(columns == wanted, logits, 0.0), axis=1, keepdims=True)
        seg = meta[:, 3:4] + 256.0 * meta[:, 4:5]
        pad = meta[:, 5:6]
        place = lax.broadcasted_iota(jnp.int32, (tokens, tokens), 0)
        block = lax.div(place, tok_dev)
        mask = jnp.zeros_like(place)
        for r, pos in enumerate(positions):
            mask = mask + (((block >> r) & 1) << pos)
        canon = (mask ^ me) * tok_dev + lax.rem(place, tok_dev)
        hit = canon == lax.broadcasted_iota(jnp.int32, (tokens, tokens), 1)
        out_ref[...] = jnp.zeros_like(out_ref)
        for row, column in enumerate((top, total, picked, seg, pad)):
            out_ref[row : row + 1, :] = jnp.sum(jnp.where(hit, column, 0.0), axis=0, keepdims=True)


def finish_kernel(all_ref, seq_ref, nll_ref, total_ref, count_ref):
    stats = all_ref[...]
    tokens = stats.shape[2]
    tops = stats[:, 0, :]
    top = jnp.max(tops, axis=0, keepdims=True)
    total = jnp.sum(stats[:, 1, :] * jnp.exp(tops - top), axis=0, keepdims=True)
    picked = jnp.sum(stats[:, 2, :], axis=0, keepdims=True)
    nll = top + jnp.log(total) - picked
    seg = all_ref[0, 3:4, :]
    pad = all_ref[0, 4:5, :]
    lane = lax.broadcasted_iota(jnp.int32, (1, tokens), 1)
    following = jnp.where(lane == tokens - 1, -1.0, pltpu.roll(seg, tokens - 1, 1))
    keep = pad * jnp.where(seg == following, 1.0, 0.0)
    count = seq_ref.shape[0]
    hot = lax.broadcasted_iota(jnp.int32, (count, tokens), 0) == seg.astype(jnp.int32)
    bench = jnp.sum(jnp.where(hot, seq_ref[...], 0), axis=0, keepdims=True)
    mine = lax.broadcasted_iota(jnp.int32, (NBENCH, tokens), 0) == bench
    nll_ref[...] = nll
    eye = lax.broadcasted_iota(jnp.int32, (NBENCH, NBENCH), 0) == lax.broadcasted_iota(jnp.int32, (NBENCH, NBENCH), 1)
    for ref, value in ((total_ref, keep * nll), (count_ref, keep)):
        column = jnp.sum(jnp.where(mine, value, 0.0), axis=1, keepdims=True)
        ref[...] = jnp.sum(jnp.where(eye, column, 0.0), axis=0, keepdims=True)


def body(hidden, lm_head, targets, segment, pad_mask, seq_bench):
    tok_dev, width = hidden.shape
    voc_dev = lm_head.shape[1]
    n_dp, n_voc = lax.axis_size("dp"), lax.axis_size("vocab")
    devices = n_dp * n_voc
    tokens = tok_dev * devices
    own_index = lax.axis_index(AXES).astype(jnp.int32)

    meta = jnp.stack(
        [digit(targets, 0), digit(targets, 1), digit(targets, 2), digit(segment, 0), digit(segment, 1), digit(pad_mask, 0)],
        axis=1,
    )
    meta = jnp.pad(meta, ((0, 0), (0, LANES - meta.shape[1])))
    half = width // 2
    order_a, order_b = gather_orders(n_dp, n_voc)
    packed = (ROWS // tok_dev).bit_length() - 1
    xa = gather_half(jnp.concatenate([hidden[:, :half], meta], axis=1), order_a, packed)
    xb = gather_half(hidden[:, half:], order_b, packed)

    blocks = xa.shape[0]
    late_a, late_b = order_a[packed:], order_b[packed:]
    spot = [late_b.index(entry) for entry in late_a]
    perm = [sum(((i >> r) & 1) << spot[r] for r in range(len(spot))) for i in range(blocks)]
    positions = [
        (bit.bit_length() - 1) + (n_voc.bit_length() - 1 if axis == "dp" else 0) for axis, bit in order_a
    ]
    steps_a = half // KTILE
    steps = width // KTILE
    stats = pl.pallas_call(
        partial(logits_kernel, perm, positions, tok_dev, steps_a),
        out_shape=jax.ShapeDtypeStruct((8, tokens), jnp.float32),
        grid_spec=pltpu.PrefetchScalarGridSpec(
            num_scalar_prefetch=1,
            grid=(steps,),
            in_specs=[
                pl.BlockSpec((blocks, ROWS, KTILE), lambda k, me: (0, 0, jnp.minimum(k, steps_a - 1))),
                pl.BlockSpec((blocks, ROWS, KTILE), lambda k, me: (0, 0, jnp.maximum(k - steps_a, 0))),
                pl.BlockSpec((blocks, ROWS, LANES), lambda k, me: (0, 0, half // LANES)),
                pl.BlockSpec((voc_dev, KTILE), lambda k, me: (0, k)),
            ],
            out_specs=pl.BlockSpec((8, tokens), lambda k, me: (0, 0)),
            scratch_shapes=[
                pltpu.VMEM((tokens, KTILE), jnp.bfloat16),
                pltpu.VMEM((tokens, voc_dev), jnp.float32),
            ],
        ),
        compiler_params=pltpu.CompilerParams(dimension_semantics=("arbitrary",), vmem_limit_bytes=24 * 1024 * 1024),
        cost_estimate=pl.CostEstimate(
            flops=2 * tokens * width * voc_dev, bytes_accessed=2 * width * voc_dev, transcendentals=tokens * voc_dev
        ),
        name="logits_stats",
    )(own_index.reshape(1), xa, xb, xa, lm_head.T)

    spread = jnp.broadcast_to(stats[None], (devices,) + stats.shape)
    gathered = lax.all_to_all(spread, AXES, split_axis=0, concat_axis=0, tiled=True)
    nll, bench_total, bench_count = pl.pallas_call(
        finish_kernel,
        out_shape=(
            jax.ShapeDtypeStruct((1, tokens), jnp.float32),
            jax.ShapeDtypeStruct((1, NBENCH), jnp.float32),
            jax.ShapeDtypeStruct((1, NBENCH), jnp.float32),
        ),
        name="finish",
    )(gathered, seq_bench.reshape(-1, 1))
    token_nll = lax.dynamic_slice_in_dim(nll.reshape(tokens), own_index * tok_dev, tok_dev, 0)
    return (token_nll, bench_total.reshape(NBENCH), bench_count.reshape(NBENCH))


def solution(mesh):
    in_specs = (
        P(AXES, None),
        P(None, AXES),
        P(AXES),
        P(AXES),
        P(AXES),
        P(),
    )
    out_specs = (P(AXES), P(), P())
    return jax.shard_map(body, mesh=mesh, in_specs=in_specs, out_specs=out_specs, check_vma=False)
```
